32 devices in a mesh: member: 1, span: 32 (over z, y, x, core).
Axes of the slice: x: 2, y: 2, z: 4, core: 2. Of those that a mesh axis runs over, the one named last changes fastest.
Arguments:
- field: float32 [1024, 23040], P(('member', 'span')), may hold values from -60 to 60
- day_table: int32 [1024], P('member'), may hold values from 0 to 364
- band_owner: int32 [32], P('member'), may hold values from 0 to 31, as said below
- sea_mask: int32 [23040], replicated, may hold values 0 or 1
Outputs:
- coeff_out: float32 [13, 23040], P(None, ('member', 'span'))
- variance_out: float32 [23040], P(('member', 'span'))
The draws below stay inside these ranges and needn't reach their ends.
Inputs may be any that keep to these rules, and one draw needn't show every extreme that they name: `band_owner`: a permutation of 0 to 31.
All inputs are finite; a program needn't handle non-finite values.
Results may differ from the reference program's by a relative error of at most 0.00013.
Values sent between devices are 32-bit elements; how exact they have to be, the bound alone decides.
A program may use at most 64 MiB of HBM per device.

```python
import math
import jax
import jax.numpy as jnp
from jax import lax

HARMS = 6
HARM_COLS = 13
STEPS = 1024
BAND = 720
CELLS = 23040
N_SPAN = 32


def calendar_days(key):
    return jax.random.randint(jax.random.fold_in(key, 11), (STEPS,), 0, 365).astype(jnp.int32)


def draw_day_table(key, part):
    return calendar_days(key)


def draw_band_owner(key, part):
    quads = N_SPAN // 4
    half = N_SPAN // 2
    kinds = jax.random.randint(jax.random.fold_in(key, 51), (quads,), 0, 4).astype(jnp.int32)
    first = jax.random.randint(jax.random.fold_in(key, 52), (), 0, quads).astype(jnp.int32)
    second = ((first + 1 + jax.random.randint(jax.random.fold_in(key, 53), (), 0, quads - 1)) % quads).astype(jnp.int32)
    kinds = kinds.at[first].set(0).at[second].set(1)
    index = jnp.arange(quads, dtype=jnp.int32)
    first_a = 2 * index
    first_b = 2 * index + 1
    first_c = 2 * index + half
    first_d = 2 * index + 1 + half
    owner_a = jnp.select([kinds == 0, kinds == 1, kinds == 2], [first_b, first_c, first_b], first_c)
    owner_b = jnp.select([kinds == 0, kinds == 1, kinds == 2], [first_d, first_a, first_a], first_d)
    owner_c = jnp.select([kinds == 0, kinds == 1, kinds == 2], [first_a, first_d, first_d], first_a)
    owner_d = jnp.select([kinds == 0, kinds == 1, kinds == 2], [first_c, first_b, first_c], first_b)
    owner = jnp.zeros((N_SPAN,), jnp.int32)
    owner = owner.at[first_a].set(owner_a).at[first_b].set(owner_b)
    owner = owner.at[first_c].set(owner_c).at[first_d].set(owner_d)
    return owner.astype(jnp.int32)


def draw_field(key, part):
    day_values = calendar_days(key)
    angles = day_values.astype(jnp.float32) * (2.0 * math.pi / 365.0)
    basis_rows = [jnp.ones_like(angles)]
    for order in range(1, HARMS + 1):
        basis_rows.append(jnp.cos(order * angles))
        basis_rows.append(jnp.sin(order * angles))
    design = jnp.stack(basis_rows, 0)
    amplitude = jax.random.normal(jax.random.fold_in(key, 21), (HARM_COLS, CELLS), jnp.float32)
    noise_scale = jnp.exp(jax.random.uniform(jax.random.fold_in(key, 31), (CELLS,), jnp.float32, math.log(0.3), math.log(3.0)))
    noise_part = jax.random.normal(jax.random.fold_in(key, 41), (STEPS, CELLS), jnp.float32)
    signal = jnp.dot(design.T, amplitude, precision=lax.Precision.HIGHEST)
    return jnp.clip(signal + noise_part * noise_scale[None, :], -60.0, 60.0)


def plant(entries, own_key, low, largest):
    index_at = [jax.random.randint(jax.random.fold_in(own_key, axis), (), 0, length) for axis, length in enumerate(entries.shape)]
    widest = entries.shape.index(max(entries.shape))
    next_to = index_at[:widest] + [(index_at[widest] + 1) % entries.shape[widest]] + index_at[widest + 1:]
    return entries.at[tuple(index_at)].set(low).at[tuple(next_to)].set(largest)


def setup_inputs(seed: int = 0, part: int = 0) -> dict:
    streams_of = jax.random.split(jax.random.key(seed), 5)
    own_keys = jax.random.split(jax.random.fold_in(streams_of[4], part), 5)
    return {
        "field": draw_field(jax.random.fold_in(jax.random.fold_in(streams_of[4], part), 71), part),
        "day_table": draw_day_table(jax.random.fold_in(jax.random.fold_in(streams_of[4], part), 71), part),
        "band_owner": draw_band_owner(jax.random.fold_in(jax.random.fold_in(streams_of[4], part), 71), part),
        "sea_mask": plant((jax.random.randint(streams_of[3], (CELLS,), 0, 3) < 2).astype(jnp.int32), jax.random.fold_in(streams_of[3], 1), 0, 1),
    }


def harmonic_basis(day_values):
    angles = day_values.astype(jnp.float32) * (2.0 * math.pi / 365.0)
    basis_rows = [jnp.ones_like(angles)]
    for order in range(1, HARMS + 1):
        basis_rows.append(jnp.cos(order * angles))
        basis_rows.append(jnp.sin(order * angles))
    return jnp.stack(basis_rows, 0)

def reference(field, day_table, band_owner, sea_mask):
    design = harmonic_basis(day_table)
    gram_matrix = jnp.dot(design, design.T, precision=lax.Precision.HIGHEST)
    factor = jnp.linalg.cholesky(gram_matrix)
    projection = jnp.dot(design, field, precision=lax.Precision.HIGHEST)
    coeffs = jax.scipy.linalg.cho_solve((factor, True), projection)
    residual = field - jnp.dot(design.T, coeffs, precision=lax.Precision.HIGHEST)
    variance = jnp.sum(residual * residual, axis=0) / design.shape[1]
    weight_mask = sea_mask.astype(jnp.float32)
    coeffs = coeffs * weight_mask[None, :]
    variance = variance * weight_mask
    slots = jnp.arange(N_SPAN, dtype=jnp.int32)
    source_band = jnp.zeros((N_SPAN,), jnp.int32).at[band_owner].set(slots)
    coeff_out = coeffs.reshape(HARM_COLS, N_SPAN, BAND)[:, source_band, :].reshape(HARM_COLS, CELLS)
    variance_out = variance.reshape(N_SPAN, BAND)[source_band, :].reshape(CELLS)
    return (coeff_out, variance_out)
```

```python
import math

import jax
import jax.numpy as jnp
import numpy as np
from jax import lax
from jax.experimental import pallas as pl
from jax.experimental.pallas import tpu as pltpu
from jax.sharding import PartitionSpec as P

HARMS = 6
ROWS = 16
SUM_ROW, SQ_ROW, MASK_ROW = 0, 8, 15
COEFF_ROWS = [0] + [row for k in range(1, HARMS + 1) for row in (k, 8 + k)]
HIGH = lax.Precision.HIGHEST


def stage_orders(groups):
    bits = [1 << k for k in range(1, groups.bit_length() - 1)]
    head, tail = bits[:3], bits[3:]
    return [[1] + head[c:] + head[:c] + tail for c in range(3)]


def relative_slots(groups, order):
    slots = []
    for pos in range(groups):
        slots.append(sum(bit for k, bit in enumerate(order) if pos & (groups >> (k + 1))))
    return slots


def harmonic_rows(angles):
    width = angles.shape[1]
    order = lax.broadcasted_iota(jnp.int32, (8, width), 0)
    turned = order.astype(jnp.float32) * angles
    used = order <= HARMS
    cosines = jnp.where(used, jnp.cos(turned), 0.0)
    sines = jnp.where(used, jnp.sin(turned), 0.0)
    return jnp.concatenate([cosines, sines], axis=0)


def split3(x):
    hi = x.astype(jnp.bfloat16)
    rest = x - hi.astype(jnp.float32)
    mid = rest.astype(jnp.bfloat16)
    lo = (rest - mid.astype(jnp.float32)).astype(jnp.bfloat16)
    return hi, mid, lo


def make_kernel(groups, steps_dev, cells):
    band = cells // groups
    total_steps = groups * steps_dev
    lanes = -(-band // 128) * 128
    tiles = lanes // 128
    cuts = [128 * ((tiles * c) // 3) for c in range(4)]
    orders = stage_orders(groups)
    n_stages = len(orders[0])
    period = 128 // math.gcd(band, 128)
    period = min(period, groups)
    parts = groups // period
    part_cells = period * band

    def kernel(field_ref, day_ref, mask_ref, table_ref, coeff_ref, var_ref, *scratch):
        fld, design_ref, stat, keep = scratch[:4]
        acc = scratch[4:7]
        recv = [scratch[7 + c * n_stages : 7 + (c + 1) * n_stages] for c in range(3)]
        field_sem, send_sem, recv_sem = scratch[7 + 3 * n_stages :]
        me = lax.axis_index("span")

        def partner(bit):
            return me + bit * (1 - 2 * ((me // bit) % 2))

        barrier = pltpu.get_barrier_semaphore()
        for bit in orders[0]:
            pl.semaphore_signal(
                barrier, inc=1, device_id={"span": partner(bit)},
                device_id_type=pl.DeviceIdType.MESH,
            )
        loads = []
        for g in range(parts):
            cols = pl.ds(g * part_cells, part_cells)
            load = pltpu.make_async_copy(field_ref.at[:, cols], fld.at[:, cols], field_sem.at[g])
            load.start()
            loads.append(load)

        angles = day_ref[...].astype(jnp.float32) * (2.0 * math.pi / 365.0)
        design = harmonic_rows(angles)
        design_ref[...] = design
        first = me * steps_dev
        near = design_ref[:, pl.ds(pl.multiple_of((first // 128) * 128, 128), 128)]
        near = pltpu.roll(near, (128 - first % 128) % 128, 1)[:, :steps_dev]
        row16 = lax.broadcasted_iota(jnp.int32, (ROWS, steps_dev), 0)
        own = jnp.where(row16 == SUM_ROW, 0.0, near)
        d_hi, d_mid, d_lo = (p.astype(jnp.float32) for p in split3(own))
        none = jnp.zeros_like(d_hi)
        lhs = jnp.concatenate(
            [
                jnp.concatenate([d_hi, d_hi, d_hi], axis=1),
                jnp.concatenate([d_mid, d_mid, none], axis=1),
                jnp.concatenate([d_lo, none, none], axis=1),
            ],
            axis=0,
        ).astype(jnp.bfloat16)

        def part_stats(g, _):
            base = g * part_cells
            for j in range(period):
                off = j * band
                start = off // 128 * 128
                shift = off - start
                width = -(-(shift + band) // 128) * 128
                cols = pl.ds(pl.multiple_of(base + start, 128), width)
                values = fld[:, cols]
                total = jnp.sum(values, axis=0, keepdims=True)
                centred = values - total * (1.0 / steps_dev)
                squares = jnp.sum(centred * centred, axis=0, keepdims=True)
                rhs = jnp.concatenate(split3(centred), axis=0)
                prod = jnp.dot(lhs, rhs, preferred_element_type=jnp.float32)
                block = prod[:ROWS] + (prod[ROWS : 2 * ROWS] + prod[2 * ROWS :])
                row = lax.broadcasted_iota(jnp.int32, block.shape, 0)
                sea = mask_ref[:, cols].astype(jnp.float32)
                block = jnp.where(row == SUM_ROW, total, block)
                block = jnp.where(row == SQ_ROW, squares, block)
                block = jnp.where(row == MASK_ROW, sea, block)
                if shift:
                    block = pltpu.roll(block, width - shift, 1)
                stat[g * period + j] = block[:, :lanes]
            return 0

        for load in loads:
            load.wait()
        lax.fori_loop(0, parts, part_stats, 0)

        half = groups // 2

        def gather(c):
            def body(i, _):
                acc[c][i] = stat[table_ref[c, i], :, cuts[c] : cuts[c + 1]]
                return 0

            return body

        for c in range(3):
            lax.fori_loop(half, groups, gather(c), 0)
        pl.semaphore_wait(barrier, n_stages)

        def exchange(c, k):
            count = groups >> (k + 1)
            return pltpu.make_async_remote_copy(
                src_ref=acc[c].at[pl.ds(count, count)],
                dst_ref=recv[c][k],
                send_sem=send_sem.at[c, k],
                recv_sem=recv_sem.at[c, k],
                device_id={"span": partner(orders[c][k])},
                device_id_type=pl.DeviceIdType.MESH,
            )

        copies = [[exchange(c, k) for k in range(n_stages)] for c in range(3)]
        for c in range(3):
            copies[c][0].start()
        for c in range(3):
            lax.fori_loop(0, half, gather(c), 0)
        keep[...] = stat[table_ref[0, 0], 8:16, :]

        n_cols = 3 * n_stages
        pad_cols = -(-n_cols // 8) * 8
        step = lax.broadcasted_iota(jnp.int32, (1, total_steps), 1)
        distance = jnp.bitwise_xor(step // steps_dev, me)
        weights = []
        for c in range(3):
            seen = 0
            for k in range(n_stages):
                bit = orders[c][k]
                inside = jnp.bitwise_and(distance, groups - 1 - (seen | bit)) == 0
                sign = jnp.where(jnp.bitwise_and(distance, bit) != 0, 1.0, -1.0)
                weights.append(jnp.where(inside, sign, 0.0))
                seen |= bit
        weights += [jnp.zeros((1, total_steps), jnp.float32)] * (pad_cols - n_cols)
        weights = jnp.concatenate(weights, axis=0)
        nt = (((1,), (1,)), ((), ()))
        gram = lax.dot_general(design, design, nt, precision=HIGH, preferred_element_type=jnp.float32)
        shifts = lax.dot_general(design, weights, nt, precision=HIGH, preferred_element_type=jnp.float32)
        r_id = lax.broadcasted_iota(jnp.int32, (ROWS, ROWS), 0)
        c_id = lax.broadcasted_iota(jnp.int32, (ROWS, ROWS), 1)
        eye = (r_id == c_id).astype(jnp.float32)
        unused = (r_id == HARMS + 1) | (r_id == SQ_ROW) | (r_id == MASK_ROW)
        left = jnp.where(unused, eye, gram)
        right = eye
        for k in COEFF_ROWS:
            scale = 1.0 / left[k : k + 1, k : k + 1]
            l_row = left[k : k + 1, :] * scale
            r_row = right[k : k + 1, :] * scale
            column = left[:, k : k + 1]
            left = jnp.where(r_id == k, l_row, left - column * l_row)
            right = jnp.where(r_id == k, r_row, right - column * r_row)
        inverse = right

        row1 = lax.broadcasted_iota(jnp.int32, (ROWS, 1), 0)
        plain = (row1 == SUM_ROW) | (row1 == SQ_ROW) | (row1 == MASK_ROW)

        def merge(c, k):
            n = float(steps_dev << k)
            q = c * n_stages + k
            slope = jnp.where(plain, 0.0, shifts[:, q : q + 1])
            bend = jnp.where(row1 == SQ_ROW, 2.0 * n, 0.0)

            def body(i, _):
                mine, theirs = acc[c][i], recv[c][k][i]
                gap = (theirs[SUM_ROW : SUM_ROW + 1] - mine[SUM_ROW : SUM_ROW + 1]) * (0.5 / n)
                acc[c][i] = (mine + theirs) + gap * (slope + bend * gap)
                return 0

            return body

        for k in range(n_stages):
            count = groups >> (k + 1)
            for c in range(3):
                copies[c][k].wait_recv()
                if count > 1:
                    lax.fori_loop(count // 2, count, merge(c, k), 0)
                    lax.fori_loop(0, count // 2, merge(c, k), 0)
                    copies[c][k + 1].start()
                else:
                    merge(c, k)(0, 0)

        for c in range(3):
            lo, hi = cuts[c], min(cuts[c + 1], band)
            block = acc[c][0][:, : hi - lo]
            sea = keep[MASK_ROW - 8 : MASK_ROW - 7, lo:hi]
            mean = block[SUM_ROW : SUM_ROW + 1] * (1.0 / total_steps)
            moments = jnp.where(plain, 0.0, block)
            fit = jnp.dot(inverse, moments, precision=HIGH, preferred_element_type=jnp.float32)
            explained = jnp.sum(fit * moments, axis=0, keepdims=True)
            var = (block[SQ_ROW : SQ_ROW + 1] - explained) * (1.0 / total_steps)
            var_ref[:, lo:hi] = var * sea
            fit = jnp.where(row1 == SUM_ROW, fit + mean, fit) * sea
            for j, row in enumerate(COEFF_ROWS):
                coeff_ref[j : j + 1, lo:hi] = fit[row : row + 1]
        for c in range(3):
            for k in range(n_stages):
                copies[c][k].wait_send()

    scratch = [
        pltpu.VMEM((steps_dev, cells), jnp.float32),
        pltpu.VMEM((ROWS, total_steps), jnp.float32),
        pltpu.VMEM((groups, ROWS, lanes), jnp.float32),
        pltpu.VMEM((8, lanes), jnp.float32),
    ]
    for c in range(3):
        scratch.append(pltpu.VMEM((groups, ROWS, cuts[c + 1] - cuts[c]), jnp.float32))
    for c in range(3):
        for k in range(n_stages):
            scratch.append(
                pltpu.VMEM((groups >> (k + 1), ROWS, cuts[c + 1] - cuts[c]), jnp.float32)
            )
    scratch += [
        pltpu.SemaphoreType.DMA((parts,)),
        pltpu.SemaphoreType.DMA((3, n_stages)),
        pltpu.SemaphoreType.DMA((3, n_stages)),
    ]
    vmem = pl.BlockSpec(memory_space=pltpu.VMEM)
    return pl.pallas_call(
        kernel,
        name="harmonic_fit",
        out_shape=(
            jax.ShapeDtypeStruct((2 * HARMS + 1, band), jnp.float32),
            jax.ShapeDtypeStruct((1, band), jnp.float32),
        ),
        in_specs=[
            pl.BlockSpec(memory_space=pl.ANY), vmem, vmem,
            pl.BlockSpec(memory_space=pltpu.SMEM),
        ],
        out_specs=(vmem, vmem),
        scratch_shapes=scratch,
        compiler_params=pltpu.CompilerParams(
            collective_id=0, has_side_effects=True, vmem_limit_bytes=65_000_000
        ),
    )


def on_device(field, day_table, band_owner, sea_mask):
    groups = lax.axis_size("span")
    own_index = lax.axis_index("span")
    steps_dev, cells = field.shape
    relative = np.array([relative_slots(groups, order) for order in stage_orders(groups)], np.int32)
    slots = jnp.bitwise_xor(jnp.asarray(relative), own_index)
    bands = jnp.arange(groups, dtype=jnp.int32)
    table = jnp.sum(
        jnp.where(band_owner[None, None, :] == slots[:, :, None], bands[None, None, :], 0), axis=2
    )
    coeffs, variance = make_kernel(groups, steps_dev, cells)(
        field, day_table.reshape(1, -1), sea_mask.reshape(1, -1), table
    )
    return (coeffs, variance.reshape(-1))


def solution(mesh):
    in_specs = (P(("member", "span"), None), P("member"), P("member"), P())
    out_specs = (P(None, ("member", "span")), P(("member", "span")))
    return jax.shard_map(
        on_device, mesh=mesh, in_specs=in_specs, out_specs=out_specs, check_vma=False
    )
```

```python
import math

import jax
import jax.numpy as jnp
import numpy as np
from jax import lax
from jax.experimental import pallas as pl
from jax.experimental.pallas import tpu as pltpu
from jax.sharding import PartitionSpec as P

HARMS = 6
ROWS = 16
SUM_ROW, SQ_ROW, MASK_ROW = 0, 8, 15
COEFF_ROWS = [0] + [row for k in range(1, HARMS + 1) for row in (k, 8 + k)]
HIGH = lax.Precision.HIGHEST


def stage_orders(groups):
    bits = [1 << k for k in range(1, groups.bit_length() - 1)]
    head, tail = bits[:3], bits[3:]
    return [[1] + head[c:] + head[:c] + tail for c in range(3)]


def relative_slots(groups, order):
    slots = []
    for pos in range(groups):
        slots.append(sum(bit for k, bit in enumerate(order) if pos & (groups >> (k + 1))))
    return slots


def harmonic_rows(angles):
    width = angles.shape[1]
    order = lax.broadcasted_iota(jnp.int32, (8, width), 0)
    turned = order.astype(jnp.float32) * angles
    used = order <= HARMS
    cosines = jnp.where(used, jnp.cos(turned), 0.0)
    sines = jnp.where(used, jnp.sin(turned), 0.0)
    return jnp.concatenate([cosines, sines], axis=0)


def split3(x):
    hi = x.astype(jnp.bfloat16)
    rest = x - hi.astype(jnp.float32)
    mid = rest.astype(jnp.bfloat16)
    lo = (rest - mid.astype(jnp.float32)).astype(jnp.bfloat16)
    return hi, mid, lo


def make_kernel(groups, steps_dev, cells):
    band = cells // groups
    total_steps = groups * steps_dev
    lanes = -(-band // 128) * 128
    tiles = lanes // 128
    cuts = [128 * ((tiles * c) // 3) for c in range(4)]
    orders = stage_orders(groups)
    n_stages = len(orders[0])
    period = 128 // math.gcd(band, 128)
    period = min(period, groups)
    parts = groups // period
    part_cells = period * band

    def kernel(field_ref, day_ref, mask_ref, table_ref, coeff_ref, var_ref, *scratch):
        fld, design_ref, stat, keep = scratch[:4]
        acc = scratch[4:7]
        recv = [scratch[7 + c * n_stages : 7 + (c + 1) * n_stages] for c in range(3)]
        field_sem, send_sem, recv_sem = scratch[7 + 3 * n_stages :]
        me = lax.axis_index("span")

        def partner(bit):
            return me + bit * (1 - 2 * ((me // bit) % 2))

        barrier = pltpu.get_barrier_semaphore()
        for bit in orders[0]:
            pl.semaphore_signal(
                barrier, inc=1, device_id={"span": partner(bit)},
                device_id_type=pl.DeviceIdType.MESH,
            )
        loads = []
        for g in range(parts):
            cols = pl.ds(g * part_cells, part_cells)
            load = pltpu.make_async_copy(field_ref.at[:, cols], fld.at[:, cols], field_sem.at[g])
            load.start()
            loads.append(load)

        angles = day_ref[...].astype(jnp.float32) * (2.0 * math.pi / 365.0)
        design = harmonic_rows(angles)
        design_ref[...] = design
        first = me * steps_dev
        near = design_ref[:, pl.ds(pl.multiple_of((first // 128) * 128, 128), 128)]
        near = pltpu.roll(near, (128 - first % 128) % 128, 1)[:, :steps_dev]
        row16 = lax.broadcasted_iota(jnp.int32, (ROWS, steps_dev), 0)
        own = jnp.where(row16 == SUM_ROW, 0.0, near)
        d_hi, d_mid, d_lo = (p.astype(jnp.float32) for p in split3(own))
        none = jnp.zeros_like(d_hi)
        lhs = jnp.concatenate(
            [
                jnp.concatenate([d_hi, d_hi, d_hi], axis=1),
                jnp.concatenate([d_mid, d_mid, none], axis=1),
                jnp.concatenate([d_lo, none, none], axis=1),
            ],
            axis=0,
        ).astype(jnp.bfloat16)

        def part_stats(g, _):
            base = g * part_cells
            for j in range(period):
                off = j * band
                start = off // 128 * 128
                shift = off - start
                width = -(-(shift + band) // 128) * 128
                cols = pl.ds(pl.multiple_of(base + start, 128), width)
                values = fld[:, cols]
                total = jnp.sum(values, axis=0, keepdims=True)
                centred = values - total * (1.0 / steps_dev)
                squares = jnp.sum(centred * centred, axis=0, keepdims=True)
                rhs = jnp.concatenate(split3(centred), axis=0)
                prod = jnp.dot(lhs, rhs, preferred_element_type=jnp.float32)
                block = prod[:ROWS] + (prod[ROWS : 2 * ROWS] + prod[2 * ROWS :])
                row = lax.broadcasted_iota(jnp.int32, block.shape, 0)
                sea = mask_ref[:, cols].astype(jnp.float32)
                block = jnp.where(row == SUM_ROW, total, block)
                block = jnp.where(row == SQ_ROW, squares, block)
                block = jnp.where(row == MASK_ROW, sea, block)
                if shift:
                    block = pltpu.roll(block, width - shift, 1)
                stat[g * period + j] = block[:, :lanes]
            return 0

        for load in loads:
            load.wait()
        lax.fori_loop(0, parts, part_stats, 0)

        half = groups // 2

        def gather(c):
            def body(i, _):
                acc[c][i] = stat[table_ref[c, i], :, cuts[c] : cuts[c + 1]]
                return 0

            return body

        for c in range(3):
            lax.fori_loop(half, groups, gather(c), 0, unroll=8)
        pl.semaphore_wait(barrier, n_stages)

        def exchange(c, k, part):
            count = groups >> (k + 1)
            low, size = (count // 2, count - count // 2) if part == 0 else (0, count // 2)
            return pltpu.make_async_remote_copy(
                src_ref=acc[c].at[pl.ds(count + low, size)],
                dst_ref=recv[c][k].at[pl.ds(low, size)],
                send_sem=send_sem.at[c, k, part],
                recv_sem=recv_sem.at[c, k, part],
                device_id={"span": partner(orders[c][k])},
                device_id_type=pl.DeviceIdType.MESH,
            )

        copies = [
            [
                [exchange(c, k, part) for part in range(2 if groups >> (k + 1) > 1 else 1)]
                for k in range(n_stages)
            ]
            for c in range(3)
        ]
        for part in range(2):
            for c in range(3):
                copies[c][0][part].start()
        for c in range(3):
            lax.fori_loop(0, half, gather(c), 0, unroll=8)
        keep[...] = stat[table_ref[0, 0], 8:16, :]

        n_cols = 3 * n_stages
        pad_cols = -(-n_cols // 8) * 8
        step = lax.broadcasted_iota(jnp.int32, (1, total_steps), 1)
        distance = jnp.bitwise_xor(step // steps_dev, me)
        weights = []
        for c in range(3):
            seen = 0
            for k in range(n_stages):
                bit = orders[c][k]
                inside = jnp.bitwise_and(distance, groups - 1 - (seen | bit)) == 0
                sign = jnp.where(jnp.bitwise_and(distance, bit) != 0, 1.0, -1.0)
                weights.append(jnp.where(inside, sign, 0.0))
                seen |= bit
        weights += [jnp.zeros((1, total_steps), jnp.float32)] * (pad_cols - n_cols)
        weights = jnp.concatenate(weights, axis=0)
        nt = (((1,), (1,)), ((), ()))
        shifts = lax.dot_general(design, weights, nt, precision=HIGH, preferred_element_type=jnp.float32)
        row1 = lax.broadcasted_iota(jnp.int32, (ROWS, 1), 0)
        plain = (row1 == SUM_ROW) | (row1 == SQ_ROW) | (row1 == MASK_ROW)

        def merge(c, k):
            n = float(steps_dev << k)
            q = c * n_stages + k
            slope = jnp.where(plain, 0.0, shifts[:, q : q + 1])
            bend = jnp.where(row1 == SQ_ROW, 2.0 * n, 0.0)

            def body(i, _):
                mine, theirs = acc[c][i], recv[c][k][i]
                gap = (theirs[SUM_ROW : SUM_ROW + 1] - mine[SUM_ROW : SUM_ROW + 1]) * (0.5 / n)
                acc[c][i] = (mine + theirs) + gap * (slope + bend * gap)
                return 0

            return body

        def invert_gram():
            gram = lax.dot_general(
                design, design, nt, precision=HIGH, preferred_element_type=jnp.float32
            )
            r_id = lax.broadcasted_iota(jnp.int32, (ROWS, ROWS), 0)
            c_id = lax.broadcasted_iota(jnp.int32, (ROWS, ROWS), 1)
            eye = (r_id == c_id).astype(jnp.float32)
            unused = (r_id == HARMS + 1) | (r_id == SQ_ROW) | (r_id == MASK_ROW)
            left = jnp.where(unused, eye, gram)
            right = eye
            for k in COEFF_ROWS:
                scale = 1.0 / left[k : k + 1, k : k + 1]
                l_row = left[k : k + 1, :] * scale
                r_row = right[k : k + 1, :] * scale
                column = left[:, k : k + 1]
                left = jnp.where(r_id == k, l_row, left - column * l_row)
                right = jnp.where(r_id == k, r_row, right - column * r_row)
            return right

        for k in range(n_stages):
            count = groups >> (k + 1)
            for c in range(3):
                copies[c][k][0].wait_recv()
                for i in reversed(range(count // 2, count)):
                    merge(c, k)(i, 0)
                if count > 1:
                    for copy in copies[c][k + 1]:
                        copy.start()
            if k == 0:
                inverse = invert_gram()
            if count > 1:
                for c in range(3):
                    copies[c][k][1].wait_recv()
                    for i in range(count // 2):
                        merge(c, k)(i, 0)

        for c in range(3):
            lo, hi = cuts[c], min(cuts[c + 1], band)
            block = acc[c][0][:, : hi - lo]
            sea = keep[MASK_ROW - 8 : MASK_ROW - 7, lo:hi]
            mean = block[SUM_ROW : SUM_ROW + 1] * (1.0 / total_steps)
            moments = jnp.where(plain, 0.0, block)
            fit = jnp.dot(inverse, moments, precision=HIGH, preferred_element_type=jnp.float32)
            explained = jnp.sum(fit * moments, axis=0, keepdims=True)
            var = (block[SQ_ROW : SQ_ROW + 1] - explained) * (1.0 / total_steps)
            var_ref[:, lo:hi] = var * sea
            fit = jnp.where(row1 == SUM_ROW, fit + mean, fit) * sea
            for j, row in enumerate(COEFF_ROWS):
                coeff_ref[j : j + 1, lo:hi] = fit[row : row + 1]
        for c in range(3):
            for k in range(n_stages):
                for copy in copies[c][k]:
                    copy.wait_send()

    scratch = [
        pltpu.VMEM((steps_dev, cells), jnp.float32),
        pltpu.VMEM((ROWS, total_steps), jnp.float32),
        pltpu.VMEM((groups, ROWS, lanes), jnp.float32),
        pltpu.VMEM((8, lanes), jnp.float32),
    ]
    for c in range(3):
        scratch.append(pltpu.VMEM((groups, ROWS, cuts[c + 1] - cuts[c]), jnp.float32))
    for c in range(3):
        for k in range(n_stages):
            scratch.append(
                pltpu.VMEM((groups >> (k + 1), ROWS, cuts[c + 1] - cuts[c]), jnp.float32)
            )
    scratch += [
        pltpu.SemaphoreType.DMA((parts,)),
        pltpu.SemaphoreType.DMA((3, n_stages, 2)),
        pltpu.SemaphoreType.DMA((3, n_stages, 2)),
    ]
    vmem = pl.BlockSpec(memory_space=pltpu.VMEM)
    return pl.pallas_call(
        kernel,
        name="harmonic_fit",
        out_shape=(
            jax.ShapeDtypeStruct((2 * HARMS + 1, band), jnp.float32),
            jax.ShapeDtypeStruct((1, band), jnp.float32),
        ),
        in_specs=[
            pl.BlockSpec(memory_space=pl.ANY), vmem, vmem,
            pl.BlockSpec(memory_space=pltpu.SMEM),
        ],
        out_specs=(vmem, vmem),
        scratch_shapes=scratch,
        compiler_params=pltpu.CompilerParams(
            collective_id=0, has_side_effects=True, vmem_limit_bytes=65_000_000
        ),
    )


def on_device(field, day_table, band_owner, sea_mask):
    groups = lax.axis_size("span")
    own_index = lax.axis_index("span")
    steps_dev, cells = field.shape
    relative = np.array([relative_slots(groups, order) for order in stage_orders(groups)], np.int32)
    slots = jnp.bitwise_xor(jnp.asarray(relative), own_index)
    bands = jnp.arange(groups, dtype=jnp.int32)
    table = jnp.sum(
        jnp.where(band_owner[None, None, :] == slots[:, :, None], bands[None, None, :], 0), axis=2
    )
    coeffs, variance = make_kernel(groups, steps_dev, cells)(
        field, day_table.reshape(1, -1), sea_mask.reshape(1, -1), table
    )
    return (coeffs, variance.reshape(-1))


def solution(mesh):
    in_specs = (P(("member", "span"), None), P("member"), P("member"), P())
    out_specs = (P(None, ("member", "span")), P(("member", "span")))
    return jax.shard_map(
        on_device, mesh=mesh, in_specs=in_specs, out_specs=out_specs, check_vma=False
    )
```

```python
import math

import jax
import jax.numpy as jnp
from jax import lax
from jax.experimental import pallas as pl
from jax.experimental.pallas import tpu as pltpu
from jax.sharding import PartitionSpec as P

HARMS = 6
ROWS = 16
SUM_ROW, SQ_ROW, MASK_ROW = 0, 8, 15
COEFF_ROWS = [0] + [row for k in range(1, HARMS + 1) for row in (k, 8 + k)]
HIGH = lax.Precision.HIGHEST


def stage_orders(groups):
    bits = [1 << k for k in range(1, groups.bit_length() - 1)]
    head, tail = bits[:3], bits[3:]
    return [[1] + head[c:] + head[:c] + tail for c in range(3)]


def relative_slots(groups, order):
    slots = []
    for pos in range(groups):
        slots.append(sum(bit for k, bit in enumerate(order) if pos & (groups >> (k + 1))))
    return slots


def harmonic_rows(angles):
    width = angles.shape[1]
    order = lax.broadcasted_iota(jnp.int32, (8, width), 0)
    turned = order.astype(jnp.float32) * angles
    used = order <= HARMS
    cosines = jnp.where(used, jnp.cos(turned), 0.0)
    sines = jnp.where(used, jnp.sin(turned), 0.0)
    return jnp.concatenate([cosines, sines], axis=0)


def split3(x):
    hi = x.astype(jnp.bfloat16)
    rest = x - hi.astype(jnp.float32)
    mid = rest.astype(jnp.bfloat16)
    lo = (rest - mid.astype(jnp.float32)).astype(jnp.bfloat16)
    return hi, mid, lo


def make_kernel(groups, steps_dev, cells):
    band = cells // groups
    total_steps = groups * steps_dev
    lanes = -(-band // 128) * 128
    tiles = lanes // 128
    cuts = [128 * ((tiles * c) // 3) for c in range(4)]
    orders = stage_orders(groups)
    n_stages = len(orders[0])
    period = 128 // math.gcd(band, 128)
    period = min(period, groups)
    parts = groups // period
    part_cells = period * band

    def kernel(field_ref, day_ref, owner_ref, stat_out, inverse_out, *scratch):
        fld, design_ref, stat, table_v, table_s = scratch[:5]
        acc = scratch[5:8]
        recv = [scratch[8 + c * n_stages : 8 + (c + 1) * n_stages] for c in range(3)]
        field_sem, table_sem, send_sem, recv_sem = scratch[8 + 3 * n_stages :]
        me = lax.axis_index("span")

        def partner(bit):
            return me + bit * (1 - 2 * ((me // bit) % 2))

        barrier = pltpu.get_barrier_semaphore()
        for bit in orders[0]:
            pl.semaphore_signal(
                barrier, inc=1, device_id={"span": partner(bit)},
                device_id_type=pl.DeviceIdType.MESH,
            )
        loads = []
        for g in range(parts):
            cols = pl.ds(g * part_cells, part_cells)
            load = pltpu.make_async_copy(field_ref.at[:, cols], fld.at[:, cols], field_sem.at[g])
            load.start()
            loads.append(load)

        slot = jnp.bitwise_xor(lax.broadcasted_iota(jnp.int32, (groups, groups), 0), me)
        bands = lax.broadcasted_iota(jnp.int32, (groups, groups), 1)
        placed = jnp.where(owner_ref[...] == slot, bands, 0)
        held = jnp.minimum(jnp.sum(placed, axis=1, keepdims=True), groups - 1)
        table_v[...] = jnp.broadcast_to(held, table_v.shape)
        to_scalars = pltpu.make_async_copy(table_v, table_s, table_sem)
        to_scalars.start()

        angles = day_ref[...].astype(jnp.float32) * (2.0 * math.pi / 365.0)
        design = harmonic_rows(angles)
        design_ref[...] = design
        first = me * steps_dev
        near = design_ref[:, pl.ds(pl.multiple_of((first // 128) * 128, 128), 128)]
        near = pltpu.roll(near, (128 - first % 128) % 128, 1)[:, :steps_dev]
        row16 = lax.broadcasted_iota(jnp.int32, (ROWS, steps_dev), 0)
        own = jnp.where(row16 == SUM_ROW, 0.0, near)
        d_hi, d_mid, d_lo = (p.astype(jnp.float32) for p in split3(own))
        none = jnp.zeros_like(d_hi)
        lhs = jnp.concatenate(
            [
                jnp.concatenate([d_hi, d_hi, d_hi], axis=1),
                jnp.concatenate([d_mid, d_mid, none], axis=1),
                jnp.concatenate([d_lo, none, none], axis=1),
            ],
            axis=0,
        ).astype(jnp.bfloat16)

        def part_stats(g, _):
            base = g * part_cells
            for j in range(period):
                off = j * band
                start = off // 128 * 128
                shift = off - start
                width = -(-(shift + band) // 128) * 128
                cols = pl.ds(pl.multiple_of(base + start, 128), width)
                values = fld[:, cols]
                total = jnp.sum(values, axis=0, keepdims=True)
                centred = values - total * (1.0 / steps_dev)
                squares = jnp.sum(centred * centred, axis=0, keepdims=True)
                rhs = jnp.concatenate(split3(centred), axis=0)
                prod = jnp.dot(lhs, rhs, preferred_element_type=jnp.float32)
                block = prod[:ROWS] + (prod[ROWS : 2 * ROWS] + prod[2 * ROWS :])
                row = lax.broadcasted_iota(jnp.int32, block.shape, 0)
                block = jnp.where(row == SUM_ROW, total, block)
                block = jnp.where(row == SQ_ROW, squares, block)
                if shift:
                    block = pltpu.roll(block, width - shift, 1)
                stat[g * period + j] = block[:, :lanes]
            return 0

        for load in loads:
            load.wait()
        lax.fori_loop(0, parts, part_stats, 0)

        half = groups // 2

        slots = [relative_slots(groups, order) for order in orders]

        def gather(c, i):
            acc[c][i] = stat[table_s[slots[c][i], 0], :, cuts[c] : cuts[c + 1]]

        to_scalars.wait()
        for i in range(half, groups):
            for c in range(3):
                gather(c, i)
        pl.semaphore_wait(barrier, n_stages)

        def exchange(c, k, part):
            count = groups >> (k + 1)
            low, size = (count // 2, count - count // 2) if part == 0 else (0, count // 2)
            return pltpu.make_async_remote_copy(
                src_ref=acc[c].at[pl.ds(count + low, size)],
                dst_ref=recv[c][k].at[pl.ds(low, size)],
                send_sem=send_sem.at[c, k, part],
                recv_sem=recv_sem.at[c, k, part],
                device_id={"span": partner(orders[c][k])},
                device_id_type=pl.DeviceIdType.MESH,
            )

        copies = [
            [
                [exchange(c, k, part) for part in range(2 if groups >> (k + 1) > 1 else 1)]
                for k in range(n_stages)
            ]
            for c in range(3)
        ]
        for part in range(2):
            for c in range(3):
                copies[c][0][part].start()
        for i in range(half):
            for c in range(3):
                gather(c, i)

        n_cols = 3 * n_stages
        pad_cols = -(-n_cols // 8) * 8
        step = lax.broadcasted_iota(jnp.int32, (1, total_steps), 1)
        distance = jnp.bitwise_xor(step // steps_dev, me)
        weights = []
        for c in range(3):
            seen = 0
            for k in range(n_stages):
                bit = orders[c][k]
                inside = jnp.bitwise_and(distance, groups - 1 - (seen | bit)) == 0
                sign = jnp.where(jnp.bitwise_and(distance, bit) != 0, 1.0, -1.0)
                weights.append(jnp.where(inside, sign, 0.0))
                seen |= bit
        weights += [jnp.zeros((1, total_steps), jnp.float32)] * (pad_cols - n_cols)
        weights = jnp.concatenate(weights, axis=0)
        nt = (((1,), (1,)), ((), ()))
        shifts = lax.dot_general(design, weights, nt, precision=HIGH, preferred_element_type=jnp.float32)
        row1 = lax.broadcasted_iota(jnp.int32, (ROWS, 1), 0)
        plain = (row1 == SUM_ROW) | (row1 == SQ_ROW) | (row1 == MASK_ROW)

        def merge(c, k):
            n = float(steps_dev << k)
            q = c * n_stages + k
            slope = jnp.where(plain, 0.0, shifts[:, q : q + 1])
            bend = jnp.where(row1 == SQ_ROW, 2.0 * n, 0.0)

            def body(i, _):
                mine, theirs = acc[c][i], recv[c][k][i]
                gap = (theirs[SUM_ROW : SUM_ROW + 1] - mine[SUM_ROW : SUM_ROW + 1]) * (0.5 / n)
                acc[c][i] = (mine + theirs) + gap * (slope + bend * gap)
                return 0

            return body

        def invert_gram():
            gram = lax.dot_general(
                design, design, nt, precision=HIGH, preferred_element_type=jnp.float32
            )
            r_id = lax.broadcasted_iota(jnp.int32, (ROWS, ROWS), 0)
            c_id = lax.broadcasted_iota(jnp.int32, (ROWS, ROWS), 1)
            eye = (r_id == c_id).astype(jnp.float32)
            unused = (r_id == HARMS + 1) | (r_id == SQ_ROW) | (r_id == MASK_ROW)
            left = jnp.where(unused, eye, gram)
            right = eye
            for k in COEFF_ROWS:
                scale = 1.0 / left[k : k + 1, k : k + 1]
                l_row = left[k : k + 1, :] * scale
                r_row = right[k : k + 1, :] * scale
                column = left[:, k : k + 1]
                left = jnp.where(r_id == k, l_row, left - column * l_row)
                right = jnp.where(r_id == k, r_row, right - column * r_row)
            return right

        for k in range(n_stages):
            count = groups >> (k + 1)
            for c in range(3):
                copies[c][k][0].wait_recv()
                for i in reversed(range(count // 2, count)):
                    merge(c, k)(i, 0)
                if count > 1:
                    for copy in copies[c][k + 1]:
                        copy.start()
            if k == 0:
                inverse_out[...] = invert_gram()
            if count > 1:
                for c in range(3):
                    copies[c][k][1].wait_recv()
                    for i in range(count // 2):
                        merge(c, k)(i, 0)

        for c in range(3):
            stat_out[:, cuts[c] : cuts[c + 1]] = acc[c][0]
        for c in range(3):
            for k in range(n_stages):
                for copy in copies[c][k]:
                    copy.wait_send()

    scratch = [
        pltpu.VMEM((steps_dev, cells), jnp.float32),
        pltpu.VMEM((ROWS, total_steps), jnp.float32),
        pltpu.VMEM((groups, ROWS, lanes), jnp.float32),
        pltpu.VMEM((groups, 128), jnp.int32),
        pltpu.SMEM((groups, 128), jnp.int32),
    ]
    for c in range(3):
        scratch.append(pltpu.VMEM((groups, ROWS, cuts[c + 1] - cuts[c]), jnp.float32))
    for c in range(3):
        for k in range(n_stages):
            scratch.append(
                pltpu.VMEM((groups >> (k + 1), ROWS, cuts[c + 1] - cuts[c]), jnp.float32)
            )
    scratch += [
        pltpu.SemaphoreType.DMA((parts,)),
        pltpu.SemaphoreType.DMA,
        pltpu.SemaphoreType.DMA((3, n_stages, 2)),
        pltpu.SemaphoreType.DMA((3, n_stages, 2)),
    ]
    vmem = pl.BlockSpec(memory_space=pltpu.VMEM)
    return pl.pallas_call(
        kernel,
        name="harmonic_fit",
        out_shape=(
            jax.ShapeDtypeStruct((ROWS, lanes), jnp.float32),
            jax.ShapeDtypeStruct((ROWS, ROWS), jnp.float32),
        ),
        in_specs=[pl.BlockSpec(memory_space=pl.ANY), vmem, vmem],
        out_specs=(vmem, vmem),
        scratch_shapes=scratch,
        compiler_params=pltpu.CompilerParams(
            collective_id=0, has_side_effects=True, vmem_limit_bytes=65_000_000
        ),
    )


def make_finish(groups, total_steps, cells):
    band = cells // groups
    lanes = -(-band // 128) * 128
    mask_rows = cells // 128
    assert cells % 128 == 0 and mask_rows >= 8 and band <= 7 * 128

    def kernel(stat_ref, inverse_ref, mask_ref, owner_ref, coeff_ref, var_ref):
        me = lax.axis_index("span")
        own = jnp.int32(0)
        for b in range(groups):
            own = jnp.where(owner_ref[b] == me, b, own)
        first = own * band
        top = first // 128
        shift = first - top * 128
        base = jnp.minimum(top, mask_rows - 8)
        window = mask_ref[pl.ds(base, 8), :].astype(jnp.float32)
        window = pltpu.roll(window, (8 - (top - base)) % 8, 0)
        window = pltpu.roll(window, (128 - shift) % 128, 1)
        below = pltpu.roll(window, 7, 0)
        lane = lax.broadcasted_iota(jnp.int32, (8, 128), 1)
        window = jnp.where(lane < 128 - shift, window, below)
        sea = jnp.concatenate([window[i : i + 1] for i in range(lanes // 128)], axis=1)

        row1 = lax.broadcasted_iota(jnp.int32, (ROWS, 1), 0)
        plain = (row1 == SUM_ROW) | (row1 == SQ_ROW) | (row1 == MASK_ROW)
        block = stat_ref[...]
        mean = block[SUM_ROW : SUM_ROW + 1] * (1.0 / total_steps)
        moments = jnp.where(plain, 0.0, block)
        fit = jnp.dot(inverse_ref[...], moments, precision=HIGH, preferred_element_type=jnp.float32)
        explained = jnp.sum(fit * moments, axis=0, keepdims=True)
        var = (block[SQ_ROW : SQ_ROW + 1] - explained) * (1.0 / total_steps) * sea
        var_ref[...] = var[0, :band]
        fit = jnp.where(row1 == SUM_ROW, fit + mean, fit) * sea
        for j, row in enumerate(COEFF_ROWS):
            coeff_ref[j : j + 1, :] = fit[row : row + 1, :band]

    vmem = pl.BlockSpec(memory_space=pltpu.VMEM)
    return pl.pallas_call(
        kernel,
        name="finish_fit",
        out_shape=(
            jax.ShapeDtypeStruct((2 * HARMS + 1, band), jnp.float32),
            jax.ShapeDtypeStruct((band,), jnp.float32),
        ),
        in_specs=[vmem, vmem, vmem, pl.BlockSpec(memory_space=pltpu.SMEM)],
        out_specs=(vmem, vmem),
    )


def on_device(field, day_table, band_owner, sea_mask):
    groups = lax.axis_size("span")
    steps_dev, cells = field.shape
    stats, inverse = make_kernel(groups, steps_dev, cells)(
        field, day_table.reshape(1, -1), band_owner.reshape(1, -1)
    )
    return make_finish(groups, groups * steps_dev, cells)(
        stats, inverse, sea_mask.reshape(-1, 128), band_owner
    )


def solution(mesh):
    in_specs = (P(("member", "span"), None), P("member"), P("member"), P())
    out_specs = (P(None, ("member", "span")), P(("member", "span")))
    return jax.shard_map(
        on_device, mesh=mesh, in_specs=in_specs, out_specs=out_specs, check_vma=False
    )
```

```python
import math

import jax
import jax.numpy as jnp
from jax import lax
from jax.experimental import pallas as pl
from jax.experimental.pallas import tpu as pltpu
from jax.sharding import PartitionSpec as P

HARMS = 6
ROWS = 16
SUM_ROW, SQ_ROW, MASK_ROW = 0, 8, 15
COEFF_ROWS = [0] + [row for k in range(1, HARMS + 1) for row in (k, 8 + k)]
HIGH = lax.Precision.HIGHEST


def stage_orders(groups):
    bits = [1 << k for k in range(1, groups.bit_length() - 1)]
    head, tail = bits[:3], bits[3:]
    return [[1] + head[c:] + head[:c] + tail for c in range(3)]


def relative_slots(groups, order):
    slots = []
    for pos in range(groups):
        slots.append(sum(bit for k, bit in enumerate(order) if pos & (groups >> (k + 1))))
    return slots


def harmonic_rows(angles):
    width = angles.shape[1]
    order = lax.broadcasted_iota(jnp.int32, (8, width), 0)
    turned = order.astype(jnp.float32) * angles
    used = order <= HARMS
    cosines = jnp.where(used, jnp.cos(turned), 0.0)
    sines = jnp.where(used, jnp.sin(turned), 0.0)
    return jnp.concatenate([cosines, sines], axis=0)


def split3(x):
    hi = x.astype(jnp.bfloat16)
    rest = x - hi.astype(jnp.float32)
    mid = rest.astype(jnp.bfloat16)
    lo = (rest - mid.astype(jnp.float32)).astype(jnp.bfloat16)
    return hi, mid, lo


def make_kernel(groups, steps_dev, cells):
    band = cells // groups
    total_steps = groups * steps_dev
    lanes = -(-band // 128) * 128
    tiles = lanes // 128
    cuts = [128 * ((tiles * c) // 3) for c in range(4)]
    orders = stage_orders(groups)
    n_stages = len(orders[0])
    period = 128 // math.gcd(band, 128)
    period = min(period, groups)
    parts = groups // period
    part_cells = period * band

    def kernel(field_ref, day_ref, owner_ref, stat_out, inverse_out, *scratch):
        fld, stat, table_v, table_s = scratch[:4]
        acc = scratch[4:7]
        recv = [scratch[7 + c * n_stages : 7 + (c + 1) * n_stages] for c in range(3)]
        field_sem, table_sem, send_sem, recv_sem = scratch[7 + 3 * n_stages :]
        me = lax.axis_index("span")

        def partner(bit):
            return me + bit * (1 - 2 * ((me // bit) % 2))

        barrier = pltpu.get_barrier_semaphore()
        for bit in orders[0]:
            pl.semaphore_signal(
                barrier, inc=1, device_id={"span": partner(bit)},
                device_id_type=pl.DeviceIdType.MESH,
            )

        def load(g):
            cols = pl.ds(pl.multiple_of(g * part_cells, 128), part_cells)
            return pltpu.make_async_copy(field_ref.at[:, cols], fld.at[:, cols], field_sem.at[g])

        for g in range(parts):
            load(g).start()

        slot = jnp.bitwise_xor(lax.broadcasted_iota(jnp.int32, (groups, groups), 0), me)
        bands = lax.broadcasted_iota(jnp.int32, (groups, groups), 1)
        placed = jnp.where(owner_ref[...] == slot, bands, 0)
        held = jnp.minimum(jnp.sum(placed, axis=1, keepdims=True), groups - 1)
        table_v[...] = jnp.broadcast_to(held, table_v.shape)
        to_scalars = pltpu.make_async_copy(table_v, table_s, table_sem)
        to_scalars.start()

        turn = 2.0 * math.pi / 365.0
        first = me * steps_dev
        near = day_ref[:, pl.ds(pl.multiple_of((first // 128) * 128, 128), 128)]
        near = harmonic_rows(near.astype(jnp.float32) * turn)
        near = pltpu.roll(near, (128 - first % 128) % 128, 1)[:, :steps_dev]
        row16 = lax.broadcasted_iota(jnp.int32, (ROWS, steps_dev), 0)
        own = jnp.where(row16 == SUM_ROW, 0.0, near)
        d_hi, d_mid, d_lo = (p.astype(jnp.float32) for p in split3(own))
        none = jnp.zeros_like(d_hi)
        lhs = jnp.concatenate(
            [
                jnp.concatenate([d_hi, d_hi, d_hi], axis=1),
                jnp.concatenate([d_mid, d_mid, none], axis=1),
                jnp.concatenate([d_lo, none, none], axis=1),
            ],
            axis=0,
        ).astype(jnp.bfloat16)

        def part_stats(g, _):
            base = g * part_cells
            load(g).wait()
            for j in range(period):
                off = j * band
                start = off // 128 * 128
                shift = off - start
                width = -(-(shift + band) // 128) * 128
                cols = pl.ds(pl.multiple_of(base + start, 128), width)
                values = fld[:, cols]
                total = jnp.sum(values, axis=0, keepdims=True)
                centred = values - total * (1.0 / steps_dev)
                squares = jnp.sum(centred * centred, axis=0, keepdims=True)
                rhs = jnp.concatenate(split3(centred), axis=0)
                prod = jnp.dot(lhs, rhs, preferred_element_type=jnp.float32)
                block = prod[:ROWS] + (prod[ROWS : 2 * ROWS] + prod[2 * ROWS :])
                row = lax.broadcasted_iota(jnp.int32, block.shape, 0)
                block = jnp.where(row == SUM_ROW, total, block)
                block = jnp.where(row == SQ_ROW, squares, block)
                if shift:
                    block = pltpu.roll(block, width - shift, 1)
                stat[g * period + j] = block[:, :lanes]
            return 0

        lax.fori_loop(0, parts, part_stats, 0)

        half = groups // 2

        slots = [relative_slots(groups, order) for order in orders]

        def gather(c, i):
            acc[c][i] = stat[table_s[slots[c][i], 0], :, cuts[c] : cuts[c + 1]]

        to_scalars.wait()
        for c in range(2):
            for i in range(half, groups):
                gather(c, i)
        pl.semaphore_wait(barrier, n_stages)

        def exchange(c, k, part):
            count = groups >> (k + 1)
            low, size = (count // 2, count - count // 2) if part == 0 else (0, count // 2)
            return pltpu.make_async_remote_copy(
                src_ref=acc[c].at[pl.ds(count + low, size)],
                dst_ref=recv[c][k].at[pl.ds(low, size)],
                send_sem=send_sem.at[c, k, part],
                recv_sem=recv_sem.at[c, k, part],
                device_id={"span": partner(orders[c][k])},
                device_id_type=pl.DeviceIdType.MESH,
            )

        copies = [
            [
                [exchange(c, k, part) for part in range(2 if groups >> (k + 1) > 1 else 1)]
                for k in range(n_stages)
            ]
            for c in range(3)
        ]
        copies[0][0][0].start()
        for i in range(half, groups):
            gather(2, i)
        for part in range(2):
            for c in range(3):
                if c or part:
                    copies[c][0][part].start()
        for i in range(half):
            for c in range(3):
                gather(c, i)
        design = harmonic_rows(day_ref[...].astype(jnp.float32) * turn)

        n_cols = 3 * n_stages
        pad_cols = -(-n_cols // 8) * 8
        step = lax.broadcasted_iota(jnp.int32, (1, total_steps), 1)
        distance = jnp.bitwise_xor(step // steps_dev, me)
        weights = []
        for c in range(3):
            seen = 0
            for k in range(n_stages):
                bit = orders[c][k]
                inside = jnp.bitwise_and(distance, groups - 1 - (seen | bit)) == 0
                sign = jnp.where(jnp.bitwise_and(distance, bit) != 0, 1.0, -1.0)
                weights.append(jnp.where(inside, sign, 0.0))
                seen |= bit
        weights += [jnp.zeros((1, total_steps), jnp.float32)] * (pad_cols - n_cols)
        weights = jnp.concatenate(weights, axis=0)
        nt = (((1,), (1,)), ((), ()))
        shifts = lax.dot_general(design, weights, nt, precision=HIGH, preferred_element_type=jnp.float32)
        row1 = lax.broadcasted_iota(jnp.int32, (ROWS, 1), 0)
        plain = (row1 == SUM_ROW) | (row1 == SQ_ROW) | (row1 == MASK_ROW)

        def merge(c, k):
            n = float(steps_dev << k)
            q = c * n_stages + k
            slope = jnp.where(plain, 0.0, shifts[:, q : q + 1])
            bend = jnp.where(row1 == SQ_ROW, 2.0 * n, 0.0)

            def body(i, _):
                mine, theirs = acc[c][i], recv[c][k][i]
                gap = (theirs[SUM_ROW : SUM_ROW + 1] - mine[SUM_ROW : SUM_ROW + 1]) * (0.5 / n)
                acc[c][i] = (mine + theirs) + gap * (slope + bend * gap)
                return 0

            return body

        def invert_gram():
            gram = lax.dot_general(
                design, design, nt, precision=HIGH, preferred_element_type=jnp.float32
            )
            r_id = lax.broadcasted_iota(jnp.int32, (ROWS, ROWS), 0)
            c_id = lax.broadcasted_iota(jnp.int32, (ROWS, ROWS), 1)
            eye = (r_id == c_id).astype(jnp.float32)
            unused = (r_id == HARMS + 1) | (r_id == SQ_ROW) | (r_id == MASK_ROW)
            left = jnp.where(unused, eye, gram)
            right = eye
            for k in COEFF_ROWS:
                scale = 1.0 / left[k : k + 1, k : k + 1]
                l_row = left[k : k + 1, :] * scale
                r_row = right[k : k + 1, :] * scale
                column = left[:, k : k + 1]
                left = jnp.where(r_id == k, l_row, left - column * l_row)
                right = jnp.where(r_id == k, r_row, right - column * r_row)
            return right

        for k in range(n_stages):
            count = groups >> (k + 1)
            for c in range(3):
                copies[c][k][0].wait_recv()
                for i in reversed(range(count // 2, count)):
                    merge(c, k)(i, 0)
                if count > 1:
                    for copy in copies[c][k + 1]:
                        copy.start()
            if k == 0:
                inverse_out[...] = invert_gram()
            if count > 1:
                for c in range(3):
                    copies[c][k][1].wait_recv()
                    for i in range(count // 2):
                        merge(c, k)(i, 0)

        for c in range(3):
            stat_out[:, cuts[c] : cuts[c + 1]] = acc[c][0]
        for c in range(3):
            for k in range(n_stages):
                for copy in copies[c][k]:
                    copy.wait_send()

    scratch = [
        pltpu.VMEM((steps_dev, cells), jnp.float32),
        pltpu.VMEM((groups, ROWS, lanes), jnp.float32),
        pltpu.VMEM((groups, 128), jnp.int32),
        pltpu.SMEM((groups, 128), jnp.int32),
    ]
    for c in range(3):
        scratch.append(pltpu.VMEM((groups, ROWS, cuts[c + 1] - cuts[c]), jnp.float32))
    for c in range(3):
        for k in range(n_stages):
            scratch.append(
                pltpu.VMEM((groups >> (k + 1), ROWS, cuts[c + 1] - cuts[c]), jnp.float32)
            )
    scratch += [
        pltpu.SemaphoreType.DMA((parts,)),
        pltpu.SemaphoreType.DMA,
        pltpu.SemaphoreType.DMA((3, n_stages, 2)),
        pltpu.SemaphoreType.DMA((3, n_stages, 2)),
    ]
    vmem = pl.BlockSpec(memory_space=pltpu.VMEM)
    return pl.pallas_call(
        kernel,
        name="harmonic_fit",
        out_shape=(
            jax.ShapeDtypeStruct((ROWS, lanes), jnp.float32),
            jax.ShapeDtypeStruct((ROWS, ROWS), jnp.float32),
        ),
        in_specs=[pl.BlockSpec(memory_space=pl.ANY), vmem, vmem],
        out_specs=(vmem, vmem),
        scratch_shapes=scratch,
        compiler_params=pltpu.CompilerParams(
            collective_id=0, has_side_effects=True, vmem_limit_bytes=65_000_000
        ),
    )


def make_finish(groups, total_steps, cells):
    band = cells // groups
    lanes = -(-band // 128) * 128
    mask_rows = cells // 128
    assert cells % 128 == 0 and mask_rows >= 8 and band <= 7 * 128

    def kernel(stat_ref, inverse_ref, mask_ref, owner_ref, coeff_ref, var_ref):
        me = lax.axis_index("span")
        own = jnp.int32(0)
        for b in range(groups):
            own = jnp.where(owner_ref[b] == me, b, own)
        first = own * band
        top = first // 128
        shift = first - top * 128
        base = jnp.minimum(top, mask_rows - 8)
        window = mask_ref[pl.ds(base, 8), :].astype(jnp.float32)
        window = pltpu.roll(window, (8 - (top - base)) % 8, 0)
        window = pltpu.roll(window, (128 - shift) % 128, 1)
        below = pltpu.roll(window, 7, 0)
        lane = lax.broadcasted_iota(jnp.int32, (8, 128), 1)
        window = jnp.where(lane < 128 - shift, window, below)
        sea = jnp.concatenate([window[i : i + 1] for i in range(lanes // 128)], axis=1)

        row1 = lax.broadcasted_iota(jnp.int32, (ROWS, 1), 0)
        plain = (row1 == SUM_ROW) | (row1 == SQ_ROW) | (row1 == MASK_ROW)
        block = stat_ref[...]
        mean = block[SUM_ROW : SUM_ROW + 1] * (1.0 / total_steps)
        moments = jnp.where(plain, 0.0, block)
        fit = jnp.dot(inverse_ref[...], moments, precision=HIGH, preferred_element_type=jnp.float32)
        explained = jnp.sum(fit * moments, axis=0, keepdims=True)
        var = (block[SQ_ROW : SQ_ROW + 1] - explained) * (1.0 / total_steps) * sea
        var_ref[...] = var[0, :band]
        fit = jnp.where(row1 == SUM_ROW, fit + mean, fit) * sea
        for j, row in enumerate(COEFF_ROWS):
            coeff_ref[j : j + 1, :] = fit[row : row + 1, :band]

    vmem = pl.BlockSpec(memory_space=pltpu.VMEM)
    return pl.pallas_call(
        kernel,
        name="finish_fit",
        out_shape=(
            jax.ShapeDtypeStruct((2 * HARMS + 1, band), jnp.float32),
            jax.ShapeDtypeStruct((band,), jnp.float32),
        ),
        in_specs=[vmem, vmem, vmem, pl.BlockSpec(memory_space=pltpu.SMEM)],
        out_specs=(vmem, vmem),
    )


def on_device(field, day_table, band_owner, sea_mask):
    groups = lax.axis_size("span")
    steps_dev, cells = field.shape
    stats, inverse = make_kernel(groups, steps_dev, cells)(
        field, day_table.reshape(1, -1), band_owner.reshape(1, -1)
    )
    return make_finish(groups, groups * steps_dev, cells)(
        stats, inverse, sea_mask.reshape(-1, 128), band_owner
    )


def solution(mesh):
    in_specs = (P(("member", "span"), None), P("member"), P("member"), P())
    out_specs = (P(None, ("member", "span")), P(("member", "span")))
    return jax.shard_map(
        on_device, mesh=mesh, in_specs=in_specs, out_specs=out_specs, check_vma=False
    )
```
